32 devices in a mesh: dp: 8 (over z, y), mp: 4 (over x, core).
Axes of the slice: x: 2, y: 2, z: 4, core: 2. Of those that a mesh axis runs over, the one named last changes fastest.
Arguments:
- queries: bfloat16 [4096, 4096], P('dp', 'mp'), may hold values from -6 to 6
- passages: bfloat16 [4096, 4096], P('dp', 'mp'), may hold values from -6 to 6
- labels: int32 [4096], P('dp'), may hold values from 0 to 4095
- projection: bfloat16 [4096, 128], P('mp'), may hold values from -0.09375 to 0.09375
Outputs:
- loss: float32 [4096], P('dp')
- query_embed: bfloat16 [4096, 128], P('dp')
The draws below stay inside these ranges and needn't reach their ends.
All inputs are finite; a program needn't handle non-finite values.
Results may differ from the reference program's by a relative error of at most 0.0039.
Values may be sent and summed in bfloat16 or wider, within the bound.
A program may use at most 64 MiB of HBM per device.

```python
import jax
import jax.numpy as jnp
from jax import lax

D = 4096
E = 128
BATCH = 4096


def draw_states(key, salt):
    subkey = jax.random.fold_in(key, salt)
    values = jnp.clip(jax.random.normal(subkey, (BATCH, D), jnp.float32), -6.0, 6.0)
    return values


def draw_passages(key, part):
    return draw_states(key, 11).astype(jnp.bfloat16)


def draw_queries(key, part):
    values = draw_states(key, 7)
    return values.astype(jnp.bfloat16)


def set_ends(values, key, smallest, largest):
    spot = [jax.random.randint(jax.random.fold_in(key, axis), (), 0, length) for axis, length in enumerate(values.shape)]
    main_axis = values.shape.index(max(values.shape))
    neighbour = spot[:main_axis] + [(spot[main_axis] + 1) % values.shape[main_axis]] + spot[main_axis + 1:]
    return values.at[tuple(spot)].set(smallest).at[tuple(neighbour)].set(largest)


def block_levels(own_key, dims, split, smallest, high):
    factor_of, own = 1.0, jax.random.fold_in(own_key, 6)
    for position, blocks in split:
        heights = jnp.exp(jax.random.uniform(jax.random.fold_in(own, position), (blocks,), jnp.float32, smallest / len(split), high / len(split)))
        factor_of = factor_of * jnp.repeat(heights, dims[position] // blocks).reshape([-1 if axis == position else 1 for axis in range(len(dims))])
    return factor_of


def normal_values(stream_key, extent, width, reach, shards=(), kind=jnp.bfloat16):
    drawn = jax.random.normal(stream_key, extent, jnp.float32) * width
    if len(shards) > 0:
        drawn = block_levels(stream_key, extent, shards, -0.22, 0.18) * drawn
    return jnp.clip(drawn, min=-reach, max=reach).astype(kind)


def setup_inputs(seed: int = 0) -> dict:
    keys = jax.random.split(jax.random.key(seed), 5)
    queries = draw_queries(jax.random.fold_in(keys[4], 71), 0)
    passages = draw_passages(jax.random.fold_in(keys[4], 71), 0)
    labels = set_ends(jax.random.randint(keys[2], (BATCH,), 0, BATCH), jax.random.fold_in(keys[2], 1), 0, BATCH - 1).astype(jnp.int32)
    projection = normal_values(keys[3], (D, E), D ** -0.5, 0.09375, ((0, 4),))
    return {"queries": queries, "passages": passages, "labels": labels, "projection": projection}


def reference(queries, passages, labels, projection):
    query_embed = jnp.dot(queries, projection, preferred_element_type=jnp.float32).astype(jnp.bfloat16)
    passage_embed = jnp.dot(passages, projection, preferred_element_type=jnp.float32).astype(jnp.bfloat16)
    block = min(512, BATCH)
    count = BATCH // block
    query_blocks = query_embed.reshape(count, block, E)
    label_blocks = labels.reshape(count, block)

    def one_block(args):
        qblock, lblock = args
        scores = jnp.dot(qblock, passage_embed.T, preferred_element_type=jnp.float32)
        total = jax.nn.logsumexp(scores, axis=1)
        chosen = jnp.take_along_axis(scores, lblock[:, None].astype(jnp.int32), axis=1)[:, 0]
        return total - chosen

    loss = lax.map(one_block, (query_blocks, label_blocks)).reshape(BATCH)
    return loss, query_embed
```

```python
import functools

import jax
import jax.numpy as jnp
from jax import lax
from jax.experimental import pallas as pl
from jax.experimental.pallas import tpu as pltpu
from jax.sharding import PartitionSpec as P

MESH = pl.DeviceIdType.MESH


def is_power(count):
    return count & (count - 1) == 0


def flipped(me, step):
    result, bit = me, 1
    while bit <= step:
        if step & bit:
            result = result + bit - 2 * bit * (lax.div(me, bit) % 2)
        bit *= 2
    return result


def peer_to(me, step, count):
    return flipped(me, step) if is_power(count) else lax.rem(me + step, count)


def peer_from(me, step, count):
    return flipped(me, step) if is_power(count) else lax.rem(me - step + count, count)


def kernel(
    sizes,
    queries, passages, labels, projection,
    loss, embed_out,
    weights, q_rows, p_rows, q_send, p_send, q_recv, p_recv, q_all, p_all, stats,
    load_sem, w_sem, out_sem, qs_sem, qr_sem, ps_sem, pr_sem, as_sem, ar_sem, gs_sem, gr_sem, ts_sem, tr_sem,
):
    n_dp, n_mp, n_in = sizes
    n_out = n_dp // n_in
    dp, mp = lax.axis_index("dp"), lax.axis_index("mp")
    outer, inner = lax.div(dp, n_in), lax.rem(dp, n_in)
    rows = queries.shape[0]
    width = rows // n_mp

    order = list(range(n_mp - 1, -1, -1)) if n_mp < 4 else [2, 3] + list(range(4, n_mp)) + [1, 0]

    def chunk(step):
        return pl.ds(pl.multiple_of(peer_to(mp, step, n_mp) * width, width), width)

    weight_copy = pltpu.make_async_copy(projection, weights, w_sem)
    weight_copy.start()
    loads = {}
    for kind, source, held in ((0, passages, p_rows), (1, queries, q_rows)):
        for step in order:
            loads[kind, step] = pltpu.make_async_copy(
                source.at[chunk(step)], held.at[step], load_sem.at[kind, step]
            )
            loads[kind, step].start()

    def out_peer(step):
        return peer_to(outer, step, n_out) * n_in + inner

    def in_peer(step):
        return outer * n_in + peer_to(inner, step, n_in)

    barrier = pltpu.get_barrier_semaphore()
    greeted = 0
    for step in range(1, n_mp):
        pl.semaphore_signal(barrier, device_id={"mp": peer_to(mp, step, n_mp)}, device_id_type=MESH)
        greeted += 1
    for step in range(1, n_in):
        pl.semaphore_signal(barrier, device_id={"dp": in_peer(step)}, device_id_type=MESH)
        greeted += 1
    for step in range(1, n_out):
        pl.semaphore_signal(barrier, device_id={"dp": out_peer(step)}, device_id_type=MESH)
        greeted += 1

    sends = []

    def remote(source, target, send_sem, recv_sem, device):
        copy = pltpu.make_async_remote_copy(
            src_ref=source, dst_ref=target, send_sem=send_sem, recv_sem=recv_sem,
            device_id=device, device_id_type=MESH,
        )
        copy.start()
        sends.append(copy)
        return copy

    weight_copy.wait()
    own = {}
    parts = {}
    first = True
    for kind, held, send, recv, s_sem, r_sem in (
        (0, p_rows, p_send, p_recv, ps_sem, pr_sem),
        (1, q_rows, q_send, q_recv, qs_sem, qr_sem),
    ):
        for step in order:
            loads[kind, step].wait()
            part = jnp.dot(held[step], weights[...], preferred_element_type=jnp.float32)
            if step == 0:
                own[kind] = part
                continue
            send[step] = part.astype(jnp.bfloat16)
            if first:
                pl.semaphore_wait(barrier, greeted)
                first = False
            parts[kind, step] = remote(
                send.at[step], recv.at[step], s_sem.at[step], r_sem.at[step],
                {"mp": peer_to(mp, step, n_mp)},
            )
    if first:
        pl.semaphore_wait(barrier, greeted)

    def added(kind, recv):
        total = own[kind]
        for step in order:
            if step:
                parts[kind, step].wait_recv()
                total = total + recv[step].astype(jnp.float32)
        return total.astype(jnp.bfloat16)

    p_all[0, 0] = added(0, p_recv)
    arrivals = {}
    for step in range(1, n_out):
        arrivals[0, step] = remote(
            p_all.at[0, 0], p_all.at[0, step], gs_sem.at[0, step], gr_sem.at[0, step],
            {"dp": out_peer(step)},
        )

    def relay(out_step):
        for step in range(1, n_in):
            arrivals[step, out_step] = remote(
                p_all.at[0, out_step], p_all.at[step, out_step],
                gs_sem.at[step, out_step], gr_sem.at[step, out_step],
                {"dp": in_peer(step)},
            )

    relay(0)

    mine = pl.ds(pl.multiple_of(mp * width, width), width)
    q_all[mine] = added(1, q_recv)
    embeds = []
    for step in [s for s in order if s]:
        embeds.append(
            remote(
                q_all.at[mine], q_all.at[mine], as_sem.at[step], ar_sem.at[step],
                {"mp": peer_to(mp, step, n_mp)},
            )
        )
    for step in range(1, n_out):
        arrivals[0, step].wait_recv()
        relay(step)
    for copy in embeds:
        copy.wait_recv()
    out_copy = pltpu.make_async_copy(q_all, embed_out, out_sem)
    out_copy.start()

    wanted = labels[...]
    sub = 8
    local_id = lax.broadcasted_iota(jnp.int32, (width, rows), 0)

    def block(in_step, out_step):
        source = peer_from(outer, out_step, n_out) * n_in + peer_from(inner, in_step, n_in)
        scores = lax.dot_general(
            p_all[in_step, out_step], q_all[...], (((1,), (1,)), ((), ())),
            preferred_element_type=jnp.float32,
        )
        hit = local_id == wanted - (source * rows + mp * width)
        chosen = jnp.where(hit, scores, 0.0).reshape(width // sub, sub, rows).sum(axis=0)
        return scores.reshape(width // sub, sub, rows), chosen

    state = None
    for in_step in range(n_in):
        for out_step in range(n_out):
            if in_step:
                arrivals[in_step, out_step].wait_recv()
            scores, chosen = block(in_step, out_step)
            top = scores.max(axis=0)
            if state is None:
                total = jnp.exp(scores - top).sum(axis=0)
            else:
                top = jnp.maximum(top, state[0])
                total = state[1] * jnp.exp(state[0] - top) + jnp.exp(scores - top).sum(axis=0)
                chosen = chosen + state[2]
            state = (top, total, chosen)

    top = state[0].max(axis=0, keepdims=True)
    total = (state[1] * jnp.exp(state[0] - top)).sum(axis=0, keepdims=True)
    own_lse = top + jnp.log(total)
    own_chosen = state[2].sum(axis=0, keepdims=True)
    stats[0, 0:1] = own_lse
    stats[0, 1:2] = own_chosen
    news = []
    for step in [s for s in order if s]:
        news.append(
            remote(
                stats.at[0], stats.at[step], ts_sem.at[step], tr_sem.at[step],
                {"mp": peer_to(mp, step, n_mp)},
            )
        )
    for copy in news:
        copy.wait_recv()
    lses = [own_lse] + [stats[step, 0:1] for step in range(1, n_mp)]
    best = functools.reduce(jnp.maximum, lses)
    spread = sum(jnp.exp(lse - best) for lse in lses)
    picked = own_chosen + sum(stats[step, 1:2] for step in range(1, n_mp))
    loss[...] = best + jnp.log(spread) - picked
    out_copy.wait()
    for copy in sends:
        copy.wait_send()


def per_device(n_dp, n_mp, queries, passages, labels, projection):
    rows, depth = queries.shape
    embed = projection.shape[1]
    width = rows // n_mp
    n_in = 2 if n_dp % 2 == 0 else 1
    n_out = n_dp // n_in
    bf16, f32 = jnp.bfloat16, jnp.float32
    dma = pltpu.SemaphoreType.DMA
    anywhere = pl.BlockSpec(memory_space=pl.ANY)
    vmem = pl.BlockSpec(memory_space=pltpu.VMEM)
    loss, query_embed = pl.pallas_call(
        functools.partial(kernel, (n_dp, n_mp, n_in)),
        out_shape=(
            jax.ShapeDtypeStruct((1, rows), f32),
            jax.ShapeDtypeStruct((rows, embed), bf16),
        ),
        in_specs=[anywhere, anywhere, vmem, anywhere],
        out_specs=(vmem, anywhere),
        scratch_shapes=[
            pltpu.VMEM((depth, embed), bf16),
            pltpu.VMEM((n_mp, width, depth), bf16),
            pltpu.VMEM((n_mp, width, depth), bf16),
            pltpu.VMEM((n_mp, width, embed), bf16),
            pltpu.VMEM((n_mp, width, embed), bf16),
            pltpu.VMEM((n_mp, width, embed), bf16),
            pltpu.VMEM((n_mp, width, embed), bf16),
            pltpu.VMEM((rows, embed), bf16),
            pltpu.VMEM((n_in, n_out, width, embed), bf16),
            pltpu.VMEM((n_mp, 2, rows), f32),
            dma((2, n_mp)),
            dma,
            dma,
            dma((n_mp,)),
            dma((n_mp,)),
            dma((n_mp,)),
            dma((n_mp,)),
            dma((n_mp,)),
            dma((n_mp,)),
            dma((n_in, n_out)),
            dma((n_in, n_out)),
            dma((n_mp,)),
            dma((n_mp,)),
        ],
        compiler_params=pltpu.CompilerParams(collective_id=0, has_side_effects=True),
    )(queries, passages, labels.reshape(1, rows), projection)
    return loss.reshape(rows), query_embed


def solution(mesh):
    return jax.shard_map(
        functools.partial(per_device, mesh.shape["dp"], mesh.shape["mp"]),
        mesh=mesh,
        in_specs=(P("dp", "mp"), P("dp", "mp"), P("dp"), P("mp", None)),
        out_specs=(P("dp"), P("dp", None)),
        check_vma=False,
    )
```

```python
import functools

import jax
import jax.numpy as jnp
from jax import lax
from jax.experimental import pallas as pl
from jax.experimental.pallas import tpu as pltpu
from jax.sharding import PartitionSpec as P

MESH = pl.DeviceIdType.MESH
DIRECT = True


def is_power(count):
    return count & (count - 1) == 0


def flipped(me, step):
    result, bit = me, 1
    while bit <= step:
        if step & bit:
            result = result + bit - 2 * bit * (lax.div(me, bit) % 2)
        bit *= 2
    return result


def peer_to(me, step, count):
    return flipped(me, step) if is_power(count) else lax.rem(me + step, count)


def peer_from(me, step, count):
    return flipped(me, step) if is_power(count) else lax.rem(me - step + count, count)


def kernel(
    sizes,
    queries, passages, labels, projection,
    stats_out, embed_out,
    weights, q_rows, p_rows, q_send, p_send, q_recv, p_recv, q_all, p_all, stats, wanted_ref,
    load_sem, w_sem, label_sem, up_sem, down_sem, qs_sem, qr_sem, ps_sem, pr_sem, as_sem, ar_sem, gs_sem, gr_sem, ts_sem, tr_sem,
):
    n_dp, n_mp, n_in = sizes
    n_out = n_dp // n_in
    dp, mp = lax.axis_index("dp"), lax.axis_index("mp")
    outer, inner = lax.div(dp, n_in), lax.rem(dp, n_in)
    rows = queries.shape[0]
    width = rows // n_mp

    order = list(range(n_mp - 1, -1, -1)) if n_mp < 4 else [2, 3] + list(range(4, n_mp)) + [1, 0]

    def chunk(step):
        return pl.ds(pl.multiple_of(peer_to(mp, step, n_mp) * width, width), width)

    weight_copy = pltpu.make_async_copy(projection, weights, w_sem)
    weight_copy.start()
    loads = {}
    for kind, source, held in ((0, passages, p_rows), (1, queries, q_rows)):
        for step in order:
            loads[kind, step] = pltpu.make_async_copy(
                source.at[chunk(step)], held.at[step], load_sem.at[kind, step]
            )
            loads[kind, step].start()

    label_copy = pltpu.make_async_copy(labels, wanted_ref, label_sem)
    label_copy.start()

    def out_peer(step):
        return peer_to(outer, step, n_out) * n_in + inner

    def in_peer(step):
        return outer * n_in + peer_to(inner, step, n_in)

    barrier = pltpu.get_barrier_semaphore()
    greeted = 0
    for step in range(1, n_mp):
        pl.semaphore_signal(barrier, device_id={"mp": peer_to(mp, step, n_mp)}, device_id_type=MESH)
        greeted += 1
    for step in range(1, n_in):
        pl.semaphore_signal(barrier, device_id={"dp": in_peer(step)}, device_id_type=MESH)
        greeted += 1
    def along(where):
        return {"dp": where * n_in + inner}

    @pl.when(outer > 0)
    def _():
        pl.semaphore_signal(barrier, device_id=along(outer - 1), device_id_type=MESH)

    @pl.when(outer < n_out - 1)
    def _():
        pl.semaphore_signal(barrier, device_id=along(outer + 1), device_id_type=MESH)

    greeted = greeted + (outer > 0).astype(jnp.int32) + (outer < n_out - 1).astype(jnp.int32)

    begin = 0 if DIRECT else 1
    end = n_out - 1 - begin

    def open_line():
        pl.semaphore_wait(barrier, greeted)

        @pl.when((outer == begin) & (outer < n_out - 1))
        def _():
            pl.semaphore_signal(up_sem, device_id=along(outer + 1), device_id_type=MESH)

        @pl.when((outer == end) & (outer > 0))
        def _():
            pl.semaphore_signal(down_sem, device_id=along(outer - 1), device_id_type=MESH)

    def pass_on():
        @pl.when((outer > begin) & (outer < n_out - 1))
        def _():
            pl.semaphore_wait(up_sem, 1)
            pl.semaphore_signal(up_sem, device_id=along(outer + 1), device_id_type=MESH)

        @pl.when((outer < end) & (outer > 0))
        def _():
            pl.semaphore_wait(down_sem, 1)
            pl.semaphore_signal(down_sem, device_id=along(outer - 1), device_id_type=MESH)

    def close_line():
        @pl.when((outer > begin) & (outer == n_out - 1))
        def _():
            pl.semaphore_wait(up_sem, 1)

        @pl.when((outer < end) & (outer == 0))
        def _():
            pl.semaphore_wait(down_sem, 1)

    sends = []

    def remote(source, target, send_sem, recv_sem, device):
        copy = pltpu.make_async_remote_copy(
            src_ref=source, dst_ref=target, send_sem=send_sem, recv_sem=recv_sem,
            device_id=device, device_id_type=MESH,
        )
        copy.start()
        sends.append(copy)
        return copy

    weight_copy.wait()
    own = {}
    parts = {}
    first = True
    for kind, held, send, recv, s_sem, r_sem in (
        (0, p_rows, p_send, p_recv, ps_sem, pr_sem),
        (1, q_rows, q_send, q_recv, qs_sem, qr_sem),
    ):
        for step in order:
            loads[kind, step].wait()
            part = jnp.dot(held[step], weights[...], preferred_element_type=jnp.float32)
            if step == 0:
                own[kind] = part
                continue
            send[step] = part.astype(jnp.bfloat16)
            if first:
                open_line()
                first = False
            parts[kind, step] = remote(
                send.at[step], recv.at[step], s_sem.at[step], r_sem.at[step],
                {"mp": peer_to(mp, step, n_mp)},
            )
    if first:
        open_line()
    pass_on()

    def added(kind, recv):
        total = own[kind]
        for step in order:
            if step:
                parts[kind, step].wait_recv()
                total = total + recv[step].astype(jnp.float32)
        return total.astype(jnp.bfloat16)

    p_all[0, 0] = added(0, p_recv)
    close_line()
    arrivals = {}

    def share(source, in_step, out_step, device):
        arrivals[in_step, out_step] = remote(
            source, p_all.at[in_step, out_step], gs_sem.at[in_step, out_step], gr_sem.at[in_step, out_step], device
        )

    def relay(out_step):
        for step in range(1, n_in):
            share(p_all.at[0, out_step], step, out_step, {"dp": in_peer(step)})

    out_order = list(range(1, n_out))
    relay(0)
    for step in out_order:
        share(p_all.at[0, 0], 0, step, {"dp": out_peer(step)})
    if DIRECT:
        for step in out_order:
            for turn in range(1, n_in):
                device = peer_to(outer, step, n_out) * n_in + peer_to(inner, turn, n_in)
                share(p_all.at[0, 0], turn, step, {"dp": device})

    mine = pl.ds(pl.multiple_of(mp * width, width), width)
    q_all[mine] = added(1, q_recv)
    embeds = []
    for step in [s for s in order if s]:
        embeds.append(
            remote(
                q_all.at[mine], q_all.at[mine], as_sem.at[step], ar_sem.at[step],
                {"mp": peer_to(mp, step, n_mp)},
            )
        )
    if not DIRECT:
        for step in out_order:
            arrivals[0, step].wait_recv()
            relay(step)
    for copy in embeds:
        copy.wait_recv()
    embed_out[...] = q_all[...]

    label_copy.wait()
    wanted = wanted_ref[...]
    sub = 8
    local_id = lax.broadcasted_iota(jnp.int32, (width, rows), 0)

    def block(in_step, out_step):
        source = peer_from(outer, out_step, n_out) * n_in + peer_from(inner, in_step, n_in)
        scores = lax.dot_general(
            p_all[in_step, out_step], q_all[...], (((1,), (1,)), ((), ())),
            preferred_element_type=jnp.float32,
        )
        hit = local_id == wanted - (source * rows + mp * width)
        chosen = jnp.where(hit, scores, 0.0).reshape(width // sub, sub, rows).sum(axis=0)
        return scores.reshape(width // sub, sub, rows), chosen

    state = None
    for in_step in range(n_in):
        for out_step in range(n_out):
            if in_step or (out_step and DIRECT):
                arrivals[in_step, out_step].wait_recv()
            scores, chosen = block(in_step, out_step)
            top = scores.max(axis=0)
            if state is None:
                total = jnp.exp(scores - top).sum(axis=0)
            else:
                top = jnp.maximum(top, state[0])
                total = state[1] * jnp.exp(state[0] - top) + jnp.exp(scores - top).sum(axis=0)
                chosen = chosen + state[2]
            state = (top, total, chosen)

    top = state[0].max(axis=0, keepdims=True)
    total = (state[1] * jnp.exp(state[0] - top)).sum(axis=0, keepdims=True)
    own_lse = top + jnp.log(total)
    own_chosen = state[2].sum(axis=0, keepdims=True)
    stats[0, 0:1] = own_lse
    stats[0, 1:2] = own_chosen
    news = []
    for step in [s for s in order if s]:
        news.append(
            remote(
                stats.at[0], stats.at[step], ts_sem.at[step], tr_sem.at[step],
                {"mp": peer_to(mp, step, n_mp)},
            )
        )
    for copy in news:
        copy.wait_recv()
    stats_out[...] = stats[...]
    for copy in sends:
        copy.wait_send()


def finish(stats, embed, loss, embed_out):
    n_mp = stats.shape[0]
    lses = [stats[step, 0:1] for step in range(n_mp)]
    best = functools.reduce(jnp.maximum, lses)
    spread = sum(jnp.exp(lse - best) for lse in lses)
    picked = sum(stats[step, 1:2] for step in range(n_mp))
    loss[...] = best + jnp.log(spread) - picked
    embed_out[...] = embed[...]


def per_device(n_dp, n_mp, queries, passages, labels, projection):
    rows, depth = queries.shape
    embed = projection.shape[1]
    width = rows // n_mp
    n_in = 2 if n_dp % 2 == 0 else 1
    n_out = n_dp // n_in
    bf16, f32 = jnp.bfloat16, jnp.float32
    dma = pltpu.SemaphoreType.DMA
    anywhere = pl.BlockSpec(memory_space=pl.ANY)
    vmem = pl.BlockSpec(memory_space=pltpu.VMEM)
    stats, query_embed = pl.pallas_call(
        functools.partial(kernel, (n_dp, n_mp, n_in)),
        out_shape=(
            pltpu.VMEM((n_mp, 2, rows), f32),
            pltpu.VMEM((rows, embed), bf16),
        ),
        in_specs=[anywhere, anywhere, anywhere, anywhere],
        out_specs=(vmem, vmem),
        scratch_shapes=[
            pltpu.VMEM((depth, embed), bf16),
            pltpu.VMEM((n_mp, width, depth), bf16),
            pltpu.VMEM((n_mp, width, depth), bf16),
            pltpu.VMEM((n_mp, width, embed), bf16),
            pltpu.VMEM((n_mp, width, embed), bf16),
            pltpu.VMEM((n_mp, width, embed), bf16),
            pltpu.VMEM((n_mp, width, embed), bf16),
            pltpu.VMEM((rows, embed), bf16),
            pltpu.VMEM((n_in, n_out, width, embed), bf16),
            pltpu.VMEM((n_mp, 2, rows), f32),
            pltpu.VMEM((1, rows), jnp.int32),
            dma((2, n_mp)),
            dma,
            dma,
            pltpu.SemaphoreType.REGULAR,
            pltpu.SemaphoreType.REGULAR,
            dma((n_mp,)),
            dma((n_mp,)),
            dma((n_mp,)),
            dma((n_mp,)),
            dma((n_mp,)),
            dma((n_mp,)),
            dma((n_in, n_out)),
            dma((n_in, n_out)),
            dma((n_mp,)),
            dma((n_mp,)),
        ],
        compiler_params=pltpu.CompilerParams(collective_id=0, has_side_effects=True),
    )(queries, passages, labels.reshape(1, rows), projection)
    loss, query_embed = pl.pallas_call(
        finish,
        out_shape=(
            jax.ShapeDtypeStruct((1, rows), f32),
            jax.ShapeDtypeStruct((rows, embed), bf16),
        ),
        in_specs=[vmem, vmem],
        out_specs=(vmem, vmem),
        compiler_params=pltpu.CompilerParams(vmem_limit_bytes=2**21),
    )(*(pltpu.with_memory_space_constraint(a, pltpu.VMEM) for a in (stats, query_embed)))
    return loss.reshape(rows), query_embed


def solution(mesh):
    return jax.shard_map(
        functools.partial(per_device, mesh.shape["dp"], mesh.shape["mp"]),
        mesh=mesh,
        in_specs=(P("dp", "mp"), P("dp", "mp"), P("dp"), P("mp", None)),
        out_specs=(P("dp"), P("dp", None)),
        check_vma=False,
    )
```

```python
import functools

import jax
import jax.numpy as jnp
from jax import lax
from jax.experimental import pallas as pl
from jax.experimental.pallas import tpu as pltpu
from jax.sharding import PartitionSpec as P

MESH = pl.DeviceIdType.MESH
DIRECT = True


def is_power(count):
    return count & (count - 1) == 0


def flipped(me, step):
    result, bit = me, 1
    while bit <= step:
        if step & bit:
            result = result + bit - 2 * bit * (lax.div(me, bit) % 2)
        bit *= 2
    return result


def peer_to(me, step, count):
    return flipped(me, step) if is_power(count) else lax.rem(me + step, count)


def peer_from(me, step, count):
    return flipped(me, step) if is_power(count) else lax.rem(me - step + count, count)


def kernel(
    sizes,
    queries, passages, labels, projection,
    stats_out, embed_out,
    weights, q_rows, p_rows, q_send, p_send, q_recv, p_recv, q_all, p_all, stats, wanted_ref,
    load_sem, w_sem, label_sem, up_sem, down_sem, qs_sem, qr_sem, ps_sem, pr_sem, as_sem, ar_sem, gs_sem, gr_sem, ts_sem, tr_sem,
):
    n_dp, n_mp, n_in = sizes
    n_out = n_dp // n_in
    dp, mp = lax.axis_index("dp"), lax.axis_index("mp")
    outer, inner = lax.div(dp, n_in), lax.rem(dp, n_in)
    rows = queries.shape[0]
    width = rows // n_mp

    order = list(range(n_mp - 1, -1, -1)) if n_mp < 4 else [2, 3] + list(range(4, n_mp)) + [1, 0]

    def chunk(step):
        return pl.ds(pl.multiple_of(peer_to(mp, step, n_mp) * width, width), width)

    weight_copy = pltpu.make_async_copy(projection, weights, w_sem)
    weight_copy.start()
    loads = {}
    for kind, source, held in ((0, passages, p_rows), (1, queries, q_rows)):
        for step in order:
            loads[kind, step] = pltpu.make_async_copy(
                source.at[chunk(step)], held.at[step], load_sem.at[kind, step]
            )
            loads[kind, step].start()

    label_copy = pltpu.make_async_copy(labels, wanted_ref, label_sem)
    label_copy.start()

    def out_peer(step):
        return peer_to(outer, step, n_out) * n_in + inner

    def in_peer(step):
        return outer * n_in + peer_to(inner, step, n_in)

    barrier = pltpu.get_barrier_semaphore()
    greeted = 0
    for step in range(1, n_mp):
        pl.semaphore_signal(barrier, device_id={"mp": peer_to(mp, step, n_mp)}, device_id_type=MESH)
        greeted += 1
    for step in range(1, n_in):
        pl.semaphore_signal(barrier, device_id={"dp": in_peer(step)}, device_id_type=MESH)
        greeted += 1
    def along(where):
        return {"dp": where * n_in + inner}

    @pl.when(outer > 0)
    def _():
        pl.semaphore_signal(barrier, device_id=along(outer - 1), device_id_type=MESH)

    @pl.when(outer < n_out - 1)
    def _():
        pl.semaphore_signal(barrier, device_id=along(outer + 1), device_id_type=MESH)

    greeted = greeted + (outer > 0).astype(jnp.int32) + (outer < n_out - 1).astype(jnp.int32)

    begin = 0 if DIRECT else 1
    end = n_out - 1 - begin

    def open_line():
        pl.semaphore_wait(barrier, greeted)

        @pl.when((outer == begin) & (outer < n_out - 1))
        def _():
            pl.semaphore_signal(up_sem, device_id=along(outer + 1), device_id_type=MESH)

        @pl.when((outer == end) & (outer > 0))
        def _():
            pl.semaphore_signal(down_sem, device_id=along(outer - 1), device_id_type=MESH)

    def pass_on():
        @pl.when((outer > begin) & (outer < n_out - 1))
        def _():
            pl.semaphore_wait(up_sem, 1)
            pl.semaphore_signal(up_sem, device_id=along(outer + 1), device_id_type=MESH)

        @pl.when((outer < end) & (outer > 0))
        def _():
            pl.semaphore_wait(down_sem, 1)
            pl.semaphore_signal(down_sem, device_id=along(outer - 1), device_id_type=MESH)

    def close_line():
        @pl.when((outer > begin) & (outer == n_out - 1))
        def _():
            pl.semaphore_wait(up_sem, 1)

        @pl.when((outer < end) & (outer == 0))
        def _():
            pl.semaphore_wait(down_sem, 1)

    sends = []

    def remote(source, target, send_sem, recv_sem, device):
        copy = pltpu.make_async_remote_copy(
            src_ref=source, dst_ref=target, send_sem=send_sem, recv_sem=recv_sem,
            device_id=device, device_id_type=MESH,
        )
        copy.start()
        sends.append(copy)
        return copy

    weight_copy.wait()
    own = {}
    parts = {}
    first = True
    for kind, held, send, recv, s_sem, r_sem in (
        (0, p_rows, p_send, p_recv, ps_sem, pr_sem),
        (1, q_rows, q_send, q_recv, qs_sem, qr_sem),
    ):
        for step in order:
            loads[kind, step].wait()
            part = jnp.dot(held[step], weights[...], preferred_element_type=jnp.float32)
            if step == 0:
                own[kind] = part
                continue
            send[step] = part.astype(jnp.bfloat16)
            if first:
                open_line()
                first = False
            parts[kind, step] = remote(
                send.at[step], recv.at[step], s_sem.at[step], r_sem.at[step],
                {"mp": peer_to(mp, step, n_mp)},
            )
    if first:
        open_line()
    pass_on()

    def added(kind, recv):
        total = own[kind]
        for step in order:
            if step:
                parts[kind, step].wait_recv()
                total = total + recv[step].astype(jnp.float32)
        return total.astype(jnp.bfloat16)

    p_all[0, 0] = added(0, p_recv)
    close_line()
    arrivals = {}

    def share(source, in_step, out_step, device):
        arrivals[in_step, out_step] = remote(
            source, p_all.at[in_step, out_step], gs_sem.at[in_step, out_step], gr_sem.at[in_step, out_step], device
        )

    def relay(out_step):
        for step in range(1, n_in):
            share(p_all.at[0, out_step], step, out_step, {"dp": in_peer(step)})

    out_order = list(range(1, n_out))
    relayed = [step for step in out_order if not DIRECT or step < n_out - 1]
    relay(0)
    for step in out_order:
        share(p_all.at[0, 0], 0, step, {"dp": out_peer(step)})
    for step in [o for o in out_order if o not in relayed]:
        for turn in range(1, n_in):
            device = peer_to(outer, step, n_out) * n_in + peer_to(inner, turn, n_in)
            share(p_all.at[0, 0], turn, step, {"dp": device})

    mine = pl.ds(pl.multiple_of(mp * width, width), width)
    q_all[mine] = added(1, q_recv)
    embeds = []
    for step in [s for s in order if s]:
        embeds.append(
            remote(
                q_all.at[mine], q_all.at[mine], as_sem.at[step], ar_sem.at[step],
                {"mp": peer_to(mp, step, n_mp)},
            )
        )
    for step in relayed:
        arrivals[0, step].wait_recv()
        relay(step)
    for copy in embeds:
        copy.wait_recv()
    embed_out[...] = q_all[...]

    label_copy.wait()
    wanted = wanted_ref[...]
    sub = 8
    local_id = lax.broadcasted_iota(jnp.int32, (width, rows), 0)

    def block(in_step, out_step):
        source = peer_from(outer, out_step, n_out) * n_in + peer_from(inner, in_step, n_in)
        scores = lax.dot_general(
            p_all[in_step, out_step], q_all[...], (((1,), (1,)), ((), ())),
            preferred_element_type=jnp.float32,
        )
        hit = local_id == wanted - (source * rows + mp * width)
        chosen = jnp.where(hit, scores, 0.0).reshape(width // sub, sub, rows).sum(axis=0)
        return scores.reshape(width // sub, sub, rows), chosen

    state = None
    for in_step in range(n_in):
        for out_step in range(n_out):
            if in_step or (out_step and out_step not in relayed):
                arrivals[in_step, out_step].wait_recv()
            scores, chosen = block(in_step, out_step)
            top = scores.max(axis=0)
            if state is None:
                total = jnp.exp(scores - top).sum(axis=0)
            else:
                top = jnp.maximum(top, state[0])
                total = state[1] * jnp.exp(state[0] - top) + jnp.exp(scores - top).sum(axis=0)
                chosen = chosen + state[2]
            state = (top, total, chosen)

    top = state[0].max(axis=0, keepdims=True)
    total = (state[1] * jnp.exp(state[0] - top)).sum(axis=0, keepdims=True)
    own_lse = top + jnp.log(total)
    own_chosen = state[2].sum(axis=0, keepdims=True)
    stats[0, 0:1] = own_lse
    stats[0, 1:2] = own_chosen
    news = []
    for step in [s for s in order if s]:
        news.append(
            remote(
                stats.at[0], stats.at[step], ts_sem.at[step], tr_sem.at[step],
                {"mp": peer_to(mp, step, n_mp)},
            )
        )
    for copy in news:
        copy.wait_recv()
    stats_out[...] = stats[...]
    for copy in sends:
        copy.wait_send()


def finish(stats, embed, loss, embed_out):
    n_mp = stats.shape[0]
    lses = [stats[step, 0:1] for step in range(n_mp)]
    best = functools.reduce(jnp.maximum, lses)
    spread = sum(jnp.exp(lse - best) for lse in lses)
    picked = sum(stats[step, 1:2] for step in range(n_mp))
    loss[...] = best + jnp.log(spread) - picked
    embed_out[...] = embed[...]


def per_device(n_dp, n_mp, queries, passages, labels, projection):
    rows, depth = queries.shape
    embed = projection.shape[1]
    width = rows // n_mp
    n_in = 2 if n_dp % 2 == 0 else 1
    n_out = n_dp // n_in
    bf16, f32 = jnp.bfloat16, jnp.float32
    dma = pltpu.SemaphoreType.DMA
    anywhere = pl.BlockSpec(memory_space=pl.ANY)
    vmem = pl.BlockSpec(memory_space=pltpu.VMEM)
    stats, query_embed = pl.pallas_call(
        functools.partial(kernel, (n_dp, n_mp, n_in)),
        out_shape=(
            pltpu.VMEM((n_mp, 2, rows), f32),
            pltpu.VMEM((rows, embed), bf16),
        ),
        in_specs=[anywhere, anywhere, anywhere, anywhere],
        out_specs=(vmem, vmem),
        scratch_shapes=[
            pltpu.VMEM((depth, embed), bf16),
            pltpu.VMEM((n_mp, width, depth), bf16),
            pltpu.VMEM((n_mp, width, depth), bf16),
            pltpu.VMEM((n_mp, width, embed), bf16),
            pltpu.VMEM((n_mp, width, embed), bf16),
            pltpu.VMEM((n_mp, width, embed), bf16),
            pltpu.VMEM((n_mp, width, embed), bf16),
            pltpu.VMEM((rows, embed), bf16),
            pltpu.VMEM((n_in, n_out, width, embed), bf16),
            pltpu.VMEM((n_mp, 2, rows), f32),
            pltpu.VMEM((1, rows), jnp.int32),
            dma((2, n_mp)),
            dma,
            dma,
            pltpu.SemaphoreType.REGULAR,
            pltpu.SemaphoreType.REGULAR,
            dma((n_mp,)),
            dma((n_mp,)),
            dma((n_mp,)),
            dma((n_mp,)),
            dma((n_mp,)),
            dma((n_mp,)),
            dma((n_in, n_out)),
            dma((n_in, n_out)),
            dma((n_mp,)),
            dma((n_mp,)),
        ],
        compiler_params=pltpu.CompilerParams(collective_id=0, has_side_effects=True),
    )(queries, passages, labels.reshape(1, rows), projection)
    loss, query_embed = pl.pallas_call(
        finish,
        out_shape=(
            jax.ShapeDtypeStruct((1, rows), f32),
            jax.ShapeDtypeStruct((rows, embed), bf16),
        ),
        in_specs=[vmem, vmem],
        out_specs=(vmem, vmem),
        compiler_params=pltpu.CompilerParams(vmem_limit_bytes=2**21),
    )(*(pltpu.with_memory_space_constraint(a, pltpu.VMEM) for a in (stats, query_embed)))
    return loss.reshape(rows), query_embed


def solution(mesh):
    return jax.shard_map(
        functools.partial(per_device, mesh.shape["dp"], mesh.shape["mp"]),
        mesh=mesh,
        in_specs=(P("dp", "mp"), P("dp", "mp"), P("dp"), P("mp", None)),
        out_specs=(P("dp"), P("dp", None)),
        check_vma=False,
    )
```

```python
import functools

import jax
import jax.numpy as jnp
from jax import lax
from jax.experimental import pallas as pl
from jax.experimental.pallas import tpu as pltpu
from jax.sharding import PartitionSpec as P

MESH = pl.DeviceIdType.MESH
DIRECT = True


def is_power(count):
    return count & (count - 1) == 0


def flipped(me, step):
    result, bit = me, 1
    while bit <= step:
        if step & bit:
            result = result + bit - 2 * bit * (lax.div(me, bit) % 2)
        bit *= 2
    return result


def peer_to(me, step, count):
    return flipped(me, step) if is_power(count) else lax.rem(me + step, count)


def peer_from(me, step, count):
    return flipped(me, step) if is_power(count) else lax.rem(me - step + count, count)


def kernel(
    sizes,
    queries, passages, labels, projection,
    stats_out, embed_out,
    weights, q_rows, p_rows, q_send, p_send, q_recv, p_recv, q_all, p_all, stats, wanted_ref,
    load_sem, w_sem, label_sem, up_sem, down_sem, qs_sem, qr_sem, ps_sem, pr_sem, as_sem, ar_sem, gs_sem, gr_sem, ts_sem, tr_sem,
):
    n_dp, n_mp, n_in = sizes
    n_out = n_dp // n_in
    dp, mp = lax.axis_index("dp"), lax.axis_index("mp")
    outer, inner = lax.div(dp, n_in), lax.rem(dp, n_in)
    rows = queries.shape[0]
    width = rows // n_mp

    order = list(range(n_mp - 1, -1, -1)) if n_mp < 4 else [2, 3] + list(range(4, n_mp)) + [1, 0]

    def chunk(step):
        return pl.ds(pl.multiple_of(peer_to(mp, step, n_mp) * width, width), width)

    weight_copy = pltpu.make_async_copy(projection, weights, w_sem)
    weight_copy.start()
    loads = {}
    for kind, source, held in ((0, passages, p_rows), (1, queries, q_rows)):
        for step in order:
            loads[kind, step] = pltpu.make_async_copy(
                source.at[chunk(step)], held.at[step], load_sem.at[kind, step]
            )
            loads[kind, step].start()

    label_copy = pltpu.make_async_copy(labels, wanted_ref, label_sem)
    label_copy.start()

    def out_peer(step):
        return peer_to(outer, step, n_out) * n_in + inner

    def in_peer(step):
        return outer * n_in + peer_to(inner, step, n_in)

    barrier = pltpu.get_barrier_semaphore()
    greeted = 0
    for step in range(1, n_mp):
        pl.semaphore_signal(barrier, device_id={"mp": peer_to(mp, step, n_mp)}, device_id_type=MESH)
        greeted += 1
    for step in range(1, n_in):
        pl.semaphore_signal(barrier, device_id={"dp": in_peer(step)}, device_id_type=MESH)
        greeted += 1
    def along(where):
        return {"dp": where * n_in + inner}

    @pl.when(outer > 0)
    def _():
        pl.semaphore_signal(barrier, device_id=along(outer - 1), device_id_type=MESH)

    @pl.when(outer < n_out - 1)
    def _():
        pl.semaphore_signal(barrier, device_id=along(outer + 1), device_id_type=MESH)

    greeted = greeted + (outer > 0).astype(jnp.int32) + (outer < n_out - 1).astype(jnp.int32)

    begin = 0 if DIRECT else 1
    end = n_out - 1 - begin

    def open_line():
        pl.semaphore_wait(barrier, greeted)

        @pl.when((outer == begin) & (outer < n_out - 1))
        def _():
            pl.semaphore_signal(up_sem, device_id=along(outer + 1), device_id_type=MESH)

        @pl.when((outer == end) & (outer > 0))
        def _():
            pl.semaphore_signal(down_sem, device_id=along(outer - 1), device_id_type=MESH)

    def pass_on():
        @pl.when((outer > begin) & (outer < n_out - 1))
        def _():
            pl.semaphore_wait(up_sem, 1)
            pl.semaphore_signal(up_sem, device_id=along(outer + 1), device_id_type=MESH)

        @pl.when((outer < end) & (outer > 0))
        def _():
            pl.semaphore_wait(down_sem, 1)
            pl.semaphore_signal(down_sem, device_id=along(outer - 1), device_id_type=MESH)

    def close_line():
        @pl.when((outer > begin) & (outer == n_out - 1))
        def _():
            pl.semaphore_wait(up_sem, 1)

        @pl.when((outer < end) & (outer == 0))
        def _():
            pl.semaphore_wait(down_sem, 1)

    sends = []

    def remote(source, target, send_sem, recv_sem, device):
        copy = pltpu.make_async_remote_copy(
            src_ref=source, dst_ref=target, send_sem=send_sem, recv_sem=recv_sem,
            device_id=device, device_id_type=MESH,
        )
        copy.start()
        sends.append(copy)
        return copy

    weight_copy.wait()
    own = {}
    parts = {}
    first = True
    for kind, held, send, recv, s_sem, r_sem in (
        (0, p_rows, p_send, p_recv, ps_sem, pr_sem),
        (1, q_rows, q_send, q_recv, qs_sem, qr_sem),
    ):
        for step in order:
            loads[kind, step].wait()
            part = jnp.dot(held[step], weights[...], preferred_element_type=jnp.float32)
            if step == 0:
                own[kind] = part
                continue
            send[step] = part.astype(jnp.bfloat16)
            if first:
                open_line()
                first = False
            parts[kind, step] = remote(
                send.at[step], recv.at[step], s_sem.at[step], r_sem.at[step],
                {"mp": peer_to(mp, step, n_mp)},
            )
    if first:
        open_line()
    pass_on()

    def added(kind, recv):
        total = own[kind]
        for step in order:
            if step:
                parts[kind, step].wait_recv()
                total = total + recv[step].astype(jnp.float32)
        return total.astype(jnp.bfloat16)

    p_all[0, 0] = added(0, p_recv)
    arrivals = {}

    def share(source, in_step, out_step, device):
        arrivals[in_step, out_step] = remote(
            source, p_all.at[in_step, out_step], gs_sem.at[in_step, out_step], gr_sem.at[in_step, out_step], device
        )

    def relay(out_step):
        for step in range(1, n_in):
            share(p_all.at[0, out_step], step, out_step, {"dp": in_peer(step)})

    out_order = list(range(1, n_out))
    relayed = [step for step in out_order if not DIRECT or step < n_out - 1]
    relay(0)
    greeted_steps = out_order[:1] if is_power(n_out) else []
    for step in greeted_steps:
        share(p_all.at[0, 0], 0, step, {"dp": out_peer(step)})
    close_line()
    for step in out_order[len(greeted_steps):]:
        share(p_all.at[0, 0], 0, step, {"dp": out_peer(step)})
    for step in [o for o in out_order if o not in relayed]:
        for turn in range(1, n_in):
            device = peer_to(outer, step, n_out) * n_in + peer_to(inner, turn, n_in)
            share(p_all.at[0, 0], turn, step, {"dp": device})

    mine = pl.ds(pl.multiple_of(mp * width, width), width)
    q_all[mine] = added(1, q_recv)
    embeds = []
    for step in [s for s in order if s]:
        embeds.append(
            remote(
                q_all.at[mine], q_all.at[mine], as_sem.at[step], ar_sem.at[step],
                {"mp": peer_to(mp, step, n_mp)},
            )
        )
    for step in relayed:
        arrivals[0, step].wait_recv()
        relay(step)
    for copy in embeds:
        copy.wait_recv()
    embed_out[...] = q_all[...]

    label_copy.wait()
    wanted = wanted_ref[...]
    sub = 8
    local_id = lax.broadcasted_iota(jnp.int32, (width, rows), 0)

    def block(in_step, out_step):
        source = peer_from(outer, out_step, n_out) * n_in + peer_from(inner, in_step, n_in)
        scores = lax.dot_general(
            p_all[in_step, out_step], q_all[...], (((1,), (1,)), ((), ())),
            preferred_element_type=jnp.float32,
        )
        hit = local_id == wanted - (source * rows + mp * width)
        chosen = jnp.where(hit, scores, 0.0).reshape(width // sub, sub, rows).sum(axis=0)
        return scores.reshape(width // sub, sub, rows), chosen

    state = None
    for in_step in range(n_in):
        for out_step in range(n_out):
            if in_step or (out_step and out_step not in relayed):
                arrivals[in_step, out_step].wait_recv()
            scores, chosen = block(in_step, out_step)
            top = scores.max(axis=0)
            if state is None:
                total = jnp.exp(scores - top).sum(axis=0)
            else:
                top = jnp.maximum(top, state[0])
                total = state[1] * jnp.exp(state[0] - top) + jnp.exp(scores - top).sum(axis=0)
                chosen = chosen + state[2]
            state = (top, total, chosen)

    top = state[0].max(axis=0, keepdims=True)
    total = (state[1] * jnp.exp(state[0] - top)).sum(axis=0, keepdims=True)
    own_lse = top + jnp.log(total)
    own_chosen = state[2].sum(axis=0, keepdims=True)
    stats[0, 0:1] = own_lse
    stats[0, 1:2] = own_chosen
    news = []
    for step in [s for s in order if s]:
        news.append(
            remote(
                stats.at[0], stats.at[step], ts_sem.at[step], tr_sem.at[step],
                {"mp": peer_to(mp, step, n_mp)},
            )
        )
    for copy in news:
        copy.wait_recv()
    stats_out[...] = stats[...]
    for copy in sends:
        copy.wait_send()


def finish(stats, embed, loss, embed_out):
    n_mp = stats.shape[0]
    lses = [stats[step, 0:1] for step in range(n_mp)]
    best = functools.reduce(jnp.maximum, lses)
    spread = sum(jnp.exp(lse - best) for lse in lses)
    picked = sum(stats[step, 1:2] for step in range(n_mp))
    loss[...] = best + jnp.log(spread) - picked
    embed_out[...] = embed[...]


def per_device(n_dp, n_mp, queries, passages, labels, projection):
    rows, depth = queries.shape
    embed = projection.shape[1]
    width = rows // n_mp
    n_in = 2 if n_dp % 2 == 0 else 1
    n_out = n_dp // n_in
    bf16, f32 = jnp.bfloat16, jnp.float32
    dma = pltpu.SemaphoreType.DMA
    anywhere = pl.BlockSpec(memory_space=pl.ANY)
    vmem = pl.BlockSpec(memory_space=pltpu.VMEM)
    stats, query_embed = pl.pallas_call(
        functools.partial(kernel, (n_dp, n_mp, n_in)),
        out_shape=(
            pltpu.VMEM((n_mp, 2, rows), f32),
            pltpu.VMEM((rows, embed), bf16),
        ),
        in_specs=[anywhere, anywhere, anywhere, anywhere],
        out_specs=(vmem, vmem),
        scratch_shapes=[
            pltpu.VMEM((depth, embed), bf16),
            pltpu.VMEM((n_mp, width, depth), bf16),
            pltpu.VMEM((n_mp, width, depth), bf16),
            pltpu.VMEM((n_mp, width, embed), bf16),
            pltpu.VMEM((n_mp, width, embed), bf16),
            pltpu.VMEM((n_mp, width, embed), bf16),
            pltpu.VMEM((n_mp, width, embed), bf16),
            pltpu.VMEM((rows, embed), bf16),
            pltpu.VMEM((n_in, n_out, width, embed), bf16),
            pltpu.VMEM((n_mp, 2, rows), f32),
            pltpu.VMEM((1, rows), jnp.int32),
            dma((2, n_mp)),
            dma,
            dma,
            pltpu.SemaphoreType.REGULAR,
            pltpu.SemaphoreType.REGULAR,
            dma((n_mp,)),
            dma((n_mp,)),
            dma((n_mp,)),
            dma((n_mp,)),
            dma((n_mp,)),
            dma((n_mp,)),
            dma((n_in, n_out)),
            dma((n_in, n_out)),
            dma((n_mp,)),
            dma((n_mp,)),
        ],
        compiler_params=pltpu.CompilerParams(collective_id=0, has_side_effects=True),
    )(queries, passages, labels.reshape(1, rows), projection)
    loss, query_embed = pl.pallas_call(
        finish,
        out_shape=(
            jax.ShapeDtypeStruct((1, rows), f32),
            jax.ShapeDtypeStruct((rows, embed), bf16),
        ),
        in_specs=[vmem, vmem],
        out_specs=(vmem, vmem),
        compiler_params=pltpu.CompilerParams(vmem_limit_bytes=2**21),
    )(*(pltpu.with_memory_space_constraint(a, pltpu.VMEM) for a in (stats, query_embed)))
    return loss.reshape(rows), query_embed


def solution(mesh):
    return jax.shard_map(
        functools.partial(per_device, mesh.shape["dp"], mesh.shape["mp"]),
        mesh=mesh,
        in_specs=(P("dp", "mp"), P("dp", "mp"), P("dp"), P("mp", None)),
        out_specs=(P("dp"), P("dp", None)),
        check_vma=False,
    )
```
